512 devices in a mesh: gx: 8 (over z_lo), gy: 16 (over x, z_hi, core), band: 4 (over y).
Axes of the slice: x: 4, y: 4, z: 16 (z_hi: 2, z_lo: 8; z = z_hi * 8 + z_lo), core: 2. Of those that a mesh axis runs over, the one named last changes fastest.
Arguments:
- orbitals: float32 [2, 16, 64, 192, 128], P(None, 'band', 'gx', 'gy'), may hold values from -3 to 3
- external: float32 [64, 192, 128], P('gx', 'gy'), may hold values from 2 to 6
Outputs:
- orbitals_next: float32 [2, 16, 64, 192, 128], P(None, 'band', 'gx', 'gy')
- potential_next: float32 [64, 192, 128], P('gx', 'gy')
The draws below stay inside these ranges and needn't reach their ends.
All inputs are finite; a program needn't handle non-finite values.
Results may differ from the reference program's by a relative error of at most 0.00002.
Values sent between devices are 32-bit elements; how exact they have to be, the bound alone decides.
A program may use at most 64 MiB of HBM per device.

```python
import jax
import jax.numpy as jnp
from jax import lax

NZ = 128
BANDS = 16
NX = 64
NY = 192


def draw_orbitals(key, part):
    shape = (2, BANDS, NX, NY, NZ)
    first_rows = jnp.arange(NX, dtype=jnp.int32)[:, None, None]
    second_rows = jnp.arange(NY, dtype=jnp.int32)[None, :, None]
    third_rows = jnp.arange(NZ, dtype=jnp.int32)[None, None, :]
    parity = (first_rows + second_rows + third_rows) % 2
    pattern = (1 - 2 * parity).astype(jnp.float32)
    amplitude = jax.random.uniform(key, shape, jnp.float32, 0.5, 2.0)
    return (amplitude * pattern[None, None]).astype(jnp.float32)


def level_of(stream_key, shape, split, low, high):
    def one(axis_at, blocks):
        heights = jax.random.uniform(jax.random.fold_in(jax.random.fold_in(stream_key, 6), axis_at), (blocks,), jnp.float32, low / len(split), high / len(split))
        return jnp.repeat(jnp.exp(heights), shape[axis_at] // blocks).reshape((-1,) + (1,) * (len(shape) - axis_at - 1))

    loudness = one(*split[0])
    for cut in split[1:]:
        loudness = loudness * one(*cut)
    return loudness


def setup_inputs(seed: int = 0) -> dict:
    streams_of = jax.random.split(jax.random.key(seed), 3)
    return {
        "orbitals": draw_orbitals(jax.random.fold_in(streams_of[2], 71), 0),
        "external": jnp.clip(2.0 + 4.0 * jax.random.uniform(streams_of[1], (NX, NY, NZ), jnp.float32) ** level_of(streams_of[1], (NX, NY, NZ), ((0, 8), (1, 16)), -0.2, 0.2), 2.0, 6.0),
    }


step_length = 0.15
exchange_coef = 0.7386
centre_weight = -2.5
near_weight = 4.0 / 3.0
far_weight = -1.0 / 12.0


def shifted(padded, which_axis, offset):
    dimensions = padded.ndim
    selector = []
    for position in range(dimensions):
        if position < dimensions - 3:
            selector.append(slice(None))
        elif position == which_axis:
            selector.append(slice(2 + offset, padded.shape[position] - 2 + offset))
        else:
            selector.append(slice(2, padded.shape[position] - 2))
    return padded[tuple(selector)]


def laplacian(padded):
    dimensions = padded.ndim
    centre = shifted(padded, dimensions - 1, 0)
    summed = 3.0 * centre_weight * centre
    for which_axis in range(dimensions - 3, dimensions):
        summed = summed + near_weight * (shifted(padded, which_axis, 1) + shifted(padded, which_axis, -1))
        summed = summed + far_weight * (shifted(padded, which_axis, 2) + shifted(padded, which_axis, -2))
    return summed


def taylor(values, apply_fn, interval):
    summed = values
    taylor_term = values
    for degree in range(1, 5):
        image = apply_fn(taylor_term)
        factor = interval / degree
        taylor_term = jnp.stack([factor * image[1], -factor * image[0]])
        summed = summed + taylor_term
    return summed


def hamiltonian(values, potential):
    padded = jnp.pad(values, ((0, 0), (2, 2), (2, 2), (2, 2)))
    return -0.5 * laplacian(padded) + potential * values


def reference(orbitals, external):
    density_now = jnp.sum(orbitals * orbitals, axis=(0, 1))
    potential_now = external - exchange_coef * jnp.cbrt(density_now)
    by_band = jnp.moveaxis(orbitals, 1, 0)

    def apply_now(values):
        return hamiltonian(values, potential_now)

    def predict(values):
        return taylor(values, apply_now, step_length)

    predicted = lax.map(predict, by_band)
    density_next = jnp.sum(predicted * predicted, axis=(0, 1))
    potential_next = external - exchange_coef * jnp.cbrt(density_next)

    def apply_next(values):
        return hamiltonian(values, potential_next)

    def finish(values):
        halfway = taylor(values, apply_now, step_length / 2)
        return taylor(halfway, apply_next, step_length / 2)

    result = lax.map(finish, by_band)
    return jnp.moveaxis(result, 0, 1), potential_next
```

```python
import functools

import jax
import jax.numpy as jnp
from jax import lax
from jax.experimental import pallas as pl
from jax.experimental.pallas import tpu as pltpu
from jax.sharding import PartitionSpec as P

step_length = 0.15
exchange_coef = 0.7386
centre = 3.75
near_w = -2.0 / 3.0
far_w = 1.0 / 24.0

MESH = pl.DeviceIdType.MESH
F = 8
NX, NY, NZ = 8, 12, 128
H = 8
EX, EY = NX + 2 * H, NY + 2 * H


def cube_root(x):
    safe = jnp.maximum(x, 1e-37)
    y = jnp.exp(jnp.log(safe) * (1.0 / 3.0))
    y = y - (y - safe / (y * y)) * (1.0 / 3.0)
    return jnp.where(x > 1e-37, y, 0.0)


def kernel(orb, ext, out, pot, S, V, D, ys, yr, xs, xr, rs, rr, bs, br):
    gx, gy, band = lax.axis_index("gx"), lax.axis_index("gy"), lax.axis_index("band")
    n_gx, n_gy, n_band = lax.axis_size("gx"), lax.axis_size("gy"), lax.axis_size("band")
    odd = lax.rem(gy, 2)
    y_right = (odd == 0, odd == 1)
    y_gy = (gy + 1 - 2 * odd, jnp.clip(gy - 1 + 2 * odd, 0, n_gy - 1))
    far_there = (gy > 0) & (gy < n_gy - 1)
    x_gx = (jnp.maximum(gx - 1, 0), jnp.minimum(gx + 1, n_gx - 1))
    x_there = (gx > 0, gx < n_gx - 1)

    def at(x=gx, y=gy, b=band):
        return (x, y, b)

    def when_side(side, more=None):
        if side == 0:
            return pl.when(more) if more is not None else (lambda f: f())
        return pl.when(far_there & more) if more is not None else pl.when(far_there)

    bar = pltpu.get_barrier_semaphore()

    def greet(dev):
        pl.semaphore_signal(bar, inc=1, device_id=dev, device_id_type=MESH)

    count = jnp.int32(n_band)
    pl.when(far_there)(lambda: greet(at(y=y_gy[1])))
    count = count + far_there.astype(jnp.int32)
    for d in range(2):
        pl.when(x_there[d])(lambda d=d: greet(at(x=x_gx[d])))
        count = count + x_there[d].astype(jnp.int32)
    for i in range(1, n_band):
        greet(at(b=lax.rem(band + i, n_band)))
    greet(at(y=y_gy[0]))

    def density_of(u):
        return jnp.sum(u * u, axis=0, keepdims=True)

    def own_cells(body, unroll):
        def step(i, carry):
            for j in range(unroll):
                body(lax.div(i, NY // unroll), lax.rem(i, NY // unroll) * unroll + j)
            return carry

        lax.fori_loop(0, NX * (NY // unroll), step, 0)

    def take_in(x, y):
        u = orb[pl.ds(x * NY + y, F, stride=NX * NY), :]
        S[0, H + x, H + y] = u
        D[0, band, x, y] = density_of(u)

    own_cells(take_in, 4)

    zero = jnp.zeros((F, NZ), jnp.float32)

    def clear_x(x0):
        def step(i, carry):
            for slot in range(5):
                for dx in range(2):
                    S[slot, x0 + dx, i] = zero
            return carry

        lax.fori_loop(0, EY, step, 0)

    def clear_y(y0):
        def step(i, carry):
            for slot in range(5):
                for dy in range(2):
                    S[slot, i, y0 + dy] = zero
            return carry

        lax.fori_loop(0, EX, step, 0)

    pl.when(gx == 0)(lambda: clear_x(H - 2))
    pl.when(gx == n_gx - 1)(lambda: clear_x(H + NX))
    pl.when(gy == 0)(lambda: clear_y(H - 2))
    pl.when(gy == n_gy - 1)(lambda: clear_y(H + NY))

    pl.semaphore_wait(bar, count)

    def remote(src, dst, s, r, dev):
        return pltpu.make_async_remote_copy(
            src_ref=src, dst_ref=dst, send_sem=s, recv_sem=r, device_id=dev, device_id_type=MESH
        )

    def ref_of(e):
        return S.at[e] if e < 2 else V.at[e - 2]

    def y_copy(e, side, j):
        buf = ref_of(e)
        src_y = jnp.where(y_right[side], H + NY - 2 * j, H + 2 * (j - 1))
        dst_y = jnp.where(y_right[side], H - 2 * j, H + NY + 2 * (j - 1))
        return remote(
            buf.at[pl.ds(H, NX), pl.ds(src_y, 2)],
            buf.at[pl.ds(H, NX), pl.ds(dst_y, 2)],
            ys.at[e, side, j - 1],
            yr.at[e, side, j - 1],
            at(y=y_gy[side]),
        )

    def x_copy(e, d):
        buf = ref_of(e)
        depth = 8 if e < 2 else 6
        src_x = H if d == 0 else H + NX - depth
        dst_x = H + NX if d == 0 else H - depth
        return remote(
            buf.at[pl.ds(src_x, depth), pl.ds(H, NY)],
            buf.at[pl.ds(dst_x, depth), pl.ds(H, NY)],
            xs.at[e, d],
            xr.at[e, d],
            at(x=x_gx[d]),
        )

    def relay(e, side, j, d):
        buf = ref_of(e)
        depth = (8 if e < 2 else 6) - 2 * j
        y0 = jnp.where(y_right[side], H + NY + 2 * (j - 1), H - 2 * j)
        src_x = H if d == 0 else H + NX - depth
        dst_x = H + NX if d == 0 else H - depth
        return remote(
            buf.at[pl.ds(src_x, depth), pl.ds(y0, 2)],
            buf.at[pl.ds(dst_x, depth), pl.ds(y0, 2)],
            rs.at[e, side, j - 1, d],
            rr.at[e, side, j - 1, d],
            at(x=x_gx[d]),
        )

    def reach(e):
        return 4 if e < 2 else 3

    def send_y(e, side):
        @when_side(side)
        def _():
            for j in range(1, reach(e) + 1):
                y_copy(e, side, j).start()

    def send_x(e):
        for d in range(2):
            pl.when(x_there[d])(lambda d=d: x_copy(e, d).start())

    def pass_on(e, side, j):
        @when_side(side)
        def _():
            y_copy(e, side, j).wait_recv()

        if j < reach(e):
            for d in range(2):
                when_side(side, x_there[d])(lambda d=d: relay(e, side, j, d).start())

    def finish(e):
        for d in range(2):

            @pl.when(x_there[d])
            def _(d=d):
                x_copy(e, 1 - d).wait_recv()

            for side in range(2):

                @when_side(side, x_there[d])
                def _(d=d, side=side):
                    for j in range(1, reach(e)):
                        relay(e, side, j, 1 - d).wait_recv()

    def drain(e):
        for side in range(2):

            @when_side(side)
            def _(side=side):
                for j in range(1, reach(e) + 1):
                    y_copy(e, side, j).wait_send()

            for d in range(2):

                @when_side(side, x_there[d])
                def _(side=side, d=d):
                    for j in range(1, reach(e)):
                        relay(e, side, j, d).wait_send()

        for d in range(2):
            pl.when(x_there[d])(lambda d=d: x_copy(e, d).wait_send())

    def band_copy(t, i):
        return remote(
            D.at[t, band], D.at[t, band], bs.at[t, i - 1], br.at[t, i - 1], at(b=lax.rem(band + i, n_band))
        )

    def band_from(t, i):
        other = lax.rem(band + n_band - i, n_band)
        return remote(D.at[t, other], D.at[t, other], bs.at[t, i - 1], br.at[t, i - 1], at(b=other))

    lane = lax.broadcasted_iota(jnp.int32, (F, NZ), 1)
    back_1 = jnp.where(lane >= 1, near_w, 0.0)
    on_1 = jnp.where(lane < NZ - 1, near_w, 0.0)
    back_2 = jnp.where(lane >= 2, far_w, 0.0)
    on_2 = jnp.where(lane < NZ - 2, far_w, 0.0)

    def block(t, src, dst, x0, y0):
        u = {}
        for dx in range(-2, 4):
            for dy in range(-2, 6):
                if 0 <= dx < 2 or 0 <= dy < 4:
                    u[dx, dy] = S[src, x0 + dx, y0 + dy]
        for dx in range(2):
            for dy in range(4):
                c = u[dx, dy]
                one = (u[dx - 1, dy] + u[dx + 1, dy]) + (u[dx, dy - 1] + u[dx, dy + 1])
                two = (u[dx - 2, dy] + u[dx + 2, dy]) + (u[dx, dy - 2] + u[dx, dy + 2])
                along = (back_1 * pltpu.roll(c, 1, 1) + on_1 * pltpu.roll(c, NZ - 1, 1)) + (
                    back_2 * pltpu.roll(c, 2, 1) + on_2 * pltpu.roll(c, NZ - 2, 1)
                )
                S[dst, x0 + dx, y0 + dy] = (V[t, x0 + dx, y0 + dy] * c + near_w * one) + (far_w * two + along)

    def applications(t):
        def step(k, carry):
            r = 4 - k
            src = jnp.where(k == 1, t, k)

            def over_x(xp, carry):
                dx = jnp.maximum(jnp.maximum(4 - xp, xp - 7), 0)
                low = jnp.where(gy == 0, 4, 4 - (r - dx))
                high = jnp.where(gy == n_gy - 1, 10, 10 + (r - dx))

                def over_y(i, carry):
                    block(t, src, k + 1, 2 * xp, 2 * jnp.minimum(low + 2 * i, high - 2))
                    return carry

                return lax.fori_loop(0, lax.div(high - low + 1, 2), over_y, carry)

            first = jnp.where(gx == 0, 4, 4 - r)
            last = jnp.where(gx == n_gx - 1, 8, 8 + r)
            return lax.fori_loop(first, last, over_x, carry)

        lax.fori_loop(1, 5, step, 0)

    sub = lax.broadcasted_iota(jnp.int32, (F, NZ), 0)
    sign = jnp.where(sub < F // 2, 1.0, -1.0)

    def combine(s, w):
        even = w[0] + ((s**4 / 24.0) * w[4] - (s**2 / 2.0) * w[2])
        odd_part = s * w[1] - (s**3 / 6.0) * w[3]
        return even + sign * pltpu.roll(odd_part, F // 2, 0)

    def terms(t, x, y):
        return [S[t, H + x, H + y]] + [S[k, H + x, H + y] for k in range(2, 6)]

    def phase(t):
        send_y(t, 1)
        send_y(t, 0)
        for i in range(1, n_band):
            band_copy(t, i).start()
        send_x(t)
        for i in range(1, n_band):
            band_from(t, i).wait_recv()

        def to_potential(x, y):
            total = (D[t, 0, x, y] + D[t, 1, x, y]) + (D[t, 2, x, y] + D[t, 3, x, y])
            v = ext[pl.ds(x * NY + y, 1), :] - exchange_coef * cube_root(total)
            if t == 1:
                pot[pl.ds(x * NY + y, 1), :] = v
            V[t, H + x, H + y] = v + centre

        own_cells(to_potential, 4)
        send_y(t + 2, 1)
        send_y(t + 2, 0)
        send_x(t + 2)
        for j in range(1, 5):
            pass_on(t, 0, j)
        for j in range(1, 4):
            pass_on(t + 2, 0, j)
        for j in range(1, 5):
            pass_on(t, 1, j)
        for j in range(1, 4):
            pass_on(t + 2, 1, j)
        finish(t)
        finish(t + 2)
        applications(t)

    phase(0)

    def half_way(x, y):
        w = terms(0, x, y)
        D[1, band, x, y] = density_of(combine(step_length, w))
        S[1, H + x, H + y] = combine(step_length / 2, w)

    own_cells(half_way, 2)
    phase(1)

    def take_out(x, y):
        out[pl.ds(x * NY + y, F, stride=NX * NY), :] = combine(step_length / 2, terms(1, x, y))

    own_cells(take_out, 2)
    for t in range(2):
        for i in range(1, n_band):
            band_copy(t, i).wait_send()
        drain(t)
        drain(t + 2)


def body(orbitals, external):
    rows = NX * NY
    vmem = pl.BlockSpec(memory_space=pltpu.VMEM)
    dma = pltpu.SemaphoreType.DMA
    out, pot = pl.pallas_call(
        kernel,
        out_shape=(
            jax.ShapeDtypeStruct((F * rows, NZ), jnp.float32),
            jax.ShapeDtypeStruct((rows, NZ), jnp.float32),
        ),
        in_specs=[vmem, vmem],
        out_specs=(vmem, vmem),
        scratch_shapes=[
            pltpu.VMEM((6, EX, EY, F, NZ), jnp.float32),
            pltpu.VMEM((2, EX, EY, 1, NZ), jnp.float32),
            pltpu.VMEM((2, 4, NX, NY, 1, NZ), jnp.float32),
            dma((4, 2, 4)),
            dma((4, 2, 4)),
            dma((4, 2)),
            dma((4, 2)),
            dma((4, 2, 3, 2)),
            dma((4, 2, 3, 2)),
            dma((2, 3)),
            dma((2, 3)),
        ],
        compiler_params=pltpu.CompilerParams(
            collective_id=0, has_side_effects=True, vmem_limit_bytes=40 * 1024 * 1024
        ),
        name="etrs",
    )(orbitals.reshape(F * rows, NZ), external.reshape(rows, NZ))
    return out.reshape(orbitals.shape), pot.reshape(external.shape)


def solution(mesh):
    in_specs = (P(None, "band", "gx", "gy", None), P("gx", "gy", None))
    out_specs = (P(None, "band", "gx", "gy", None), P("gx", "gy", None))
    return jax.shard_map(body, mesh=mesh, in_specs=in_specs, out_specs=out_specs, check_vma=False)
```

```python
import functools

import jax
import jax.numpy as jnp
from jax import lax
from jax.experimental import pallas as pl
from jax.experimental.pallas import tpu as pltpu
from jax.sharding import PartitionSpec as P

step_length = 0.15
exchange_coef = 0.7386
centre = 3.75
far_w = 1.0 / 24.0

MESH = pl.DeviceIdType.MESH
F = 8
NX, NY, NZ = 8, 12, 128
H = 8
EX, EY = NX + 2 * H, NY + 2 * H


def cube_root(x):
    safe = jnp.maximum(x, 1e-37)
    y = jnp.exp(jnp.log(safe) * (1.0 / 3.0))
    y = y - (y - safe / (y * y)) * (1.0 / 3.0)
    return jnp.where(x > 1e-37, y, 0.0)


def scope(name):
    return lambda f: jax.named_scope(name)(f)


def kernel(orb, ext, out, pot, S, V, D, Z, ys, yr, xs, xr, rs, rr, bs, br):
    gx, gy, band = lax.axis_index("gx"), lax.axis_index("gy"), lax.axis_index("band")
    n_gx, n_gy, n_band = lax.axis_size("gx"), lax.axis_size("gy"), lax.axis_size("band")
    odd = lax.rem(gy, 2)
    y_right = (odd == 0, odd == 1)
    y_gy = (gy + 1 - 2 * odd, jnp.clip(gy - 1 + 2 * odd, 0, n_gy - 1))
    far_there = (gy > 0) & (gy < n_gy - 1)
    x_gx = (jnp.maximum(gx - 1, 0), jnp.minimum(gx + 1, n_gx - 1))
    x_there = (gx > 0, gx < n_gx - 1)

    def at(x=gx, y=gy, b=band):
        return (x, y, b)

    def when_side(side, more=None):
        if side == 0:
            return pl.when(more) if more is not None else (lambda f: f())
        return pl.when(far_there & more) if more is not None else pl.when(far_there)

    bar = pltpu.get_barrier_semaphore()

    def greet(dev):
        pl.semaphore_signal(bar, inc=1, device_id=dev, device_id_type=MESH)

    count = jnp.int32(n_band)
    pl.when(far_there)(lambda: greet(at(y=y_gy[1])))
    count = count + far_there.astype(jnp.int32)
    for d in range(2):
        pl.when(x_there[d])(lambda d=d: greet(at(x=x_gx[d])))
        count = count + x_there[d].astype(jnp.int32)
    for i in range(1, n_band):
        greet(at(b=lax.rem(band + i, n_band)))
    greet(at(y=y_gy[0]))

    def density_of(u):
        return jnp.sum(u * u, axis=0, keepdims=True)

    def own_cells(body, unroll):
        def step(i, carry):
            for j in range(unroll):
                body(lax.div(i, NY // unroll), lax.rem(i, NY // unroll) * unroll + j)
            return carry

        lax.fori_loop(0, NX * (NY // unroll), step, 0)

    def take_in(x, y):
        u = orb[pl.ds(x * NY + y, F, stride=NX * NY), :]
        S[0, H + x, H + y] = u
        D[0, band, x, y] = density_of(u)

    own_cells(take_in, 4)

    zero = jnp.zeros((F, NZ), jnp.float32)

    def clear_x(x0):
        def step(i, carry):
            for slot in range(5):
                for dx in range(2):
                    S[slot, x0 + dx, i] = zero
            return carry

        lax.fori_loop(0, EY, step, 0)

    def clear_y(y0):
        def step(i, carry):
            for slot in range(5):
                for dy in range(2):
                    S[slot, i, y0 + dy] = zero
            return carry

        lax.fori_loop(0, EX, step, 0)

    pl.when(gx == 0)(lambda: clear_x(H - 2))
    pl.when(gx == n_gx - 1)(lambda: clear_x(H + NX))
    pl.when(gy == 0)(lambda: clear_y(H - 2))
    pl.when(gy == n_gy - 1)(lambda: clear_y(H + NY))

    off = jnp.abs(lax.broadcasted_iota(jnp.int32, (NZ, NZ), 0) - lax.broadcasted_iota(jnp.int32, (NZ, NZ), 1))
    z_part = jnp.where(off == 1, -16.0, jnp.where(off == 2, 1.0, 0.0)).astype(jnp.bfloat16)
    Z[0:NZ, :] = z_part
    Z[NZ:, :] = z_part

    with jax.named_scope('barrier'):
        pl.semaphore_wait(bar, count)

    def remote(src, dst, s, r, dev):
        return pltpu.make_async_remote_copy(
            src_ref=src, dst_ref=dst, send_sem=s, recv_sem=r, device_id=dev, device_id_type=MESH
        )

    def remote(src, dst, s, r, dev):
        return pltpu.make_async_remote_copy(
            src_ref=src, dst_ref=dst, send_sem=s, recv_sem=r, device_id=dev, device_id_type=MESH
        )

    def row_of(pair):
        return jnp.where(odd == 1, H + NY - 2 - 2 * pair, H + 2 * pair)

    def ref_of(e):
        return S.at[e] if e < 2 else V.at[e - 2]

    def reach(e):
        return 4 if e < 2 else 3

    def y_copy(e, side, j):
        buf = ref_of(e)
        src_y = jnp.where(y_right[side], H + NY - 2 * j, H + 2 * (j - 1))
        dst_y = jnp.where(y_right[side], H - 2 * j, H + NY + 2 * (j - 1))
        return remote(
            buf.at[pl.ds(H, NX), pl.ds(src_y, 2)],
            buf.at[pl.ds(H, NX), pl.ds(dst_y, 2)],
            ys.at[e, side, j - 1],
            yr.at[e, side, j - 1],
            at(y=y_gy[side]),
        )

    def x_copy(e, pair, d):
        buf = ref_of(e)
        depth = 2 * reach(e)
        rows = pl.ds(row_of(pair), 2) if e < 2 else pl.ds(H, NY)
        src_x = H if d == 0 else H + NX - depth
        dst_x = H + NX if d == 0 else H - depth
        return remote(
            buf.at[pl.ds(src_x, depth), rows],
            buf.at[pl.ds(dst_x, depth), rows],
            xs.at[e, pair, d],
            xr.at[e, pair, d],
            at(x=x_gx[d]),
        )

    def relay(e, side, j, d):
        buf = ref_of(e)
        depth = 2 * (reach(e) - j)
        y0 = jnp.where(y_right[side], H + NY + 2 * (j - 1), H - 2 * j)
        src_x = H if d == 0 else H + NX - depth
        dst_x = H + NX if d == 0 else H - depth
        return remote(
            buf.at[pl.ds(src_x, depth), pl.ds(y0, 2)],
            buf.at[pl.ds(dst_x, depth), pl.ds(y0, 2)],
            rs.at[e, side, j - 1, d],
            rr.at[e, side, j - 1, d],
            at(x=x_gx[d]),
        )

    def send_y(e, side, pieces):
        @when_side(side)
        def _():
            for j in pieces:
                y_copy(e, side, j).start()

    def x_pairs(e):
        return range(NY // 2) if e < 2 else range(1)

    def send_x(e, pairs):
        for d in range(2):

            @pl.when(x_there[d])
            def _(d=d):
                for pair in pairs:
                    x_copy(e, pair, d).start()

    def pass_on(e, side, pieces):
        for j in pieces:

            @when_side(side)
            def _(j=j):
                y_copy(e, side, j).wait_recv()

            if j < reach(e):
                for d in range(2):
                    when_side(side, x_there[d])(lambda j=j, d=d: relay(e, side, j, d).start())

    def await_relay(e, side, pieces):
        for d in range(2):

            @when_side(side, x_there[d])
            def _(d=d):
                for j in pieces:
                    relay(e, side, j, 1 - d).wait_recv()

    def await_x(e):
        for d in range(2):

            @pl.when(x_there[d])
            def _(d=d):
                for pair in x_pairs(e):
                    x_copy(e, pair, 1 - d).wait_recv()

    def drain(e):
        for side in range(2):

            @when_side(side)
            def _(side=side):
                for j in range(1, reach(e) + 1):
                    y_copy(e, side, j).wait_send()

            for d in range(2):

                @when_side(side, x_there[d])
                def _(side=side, d=d):
                    for j in range(1, reach(e)):
                        relay(e, side, j, d).wait_send()

        for d in range(2):

            @pl.when(x_there[d])
            def _(d=d):
                for pair in x_pairs(e):
                    x_copy(e, pair, d).wait_send()

    def band_copy(t, i):
        return remote(
            D.at[t, band], D.at[t, band], bs.at[t, i - 1], br.at[t, i - 1], at(b=lax.rem(band + i, n_band))
        )

    def band_from(t, i):
        other = lax.rem(band + n_band - i, n_band)
        return remote(D.at[t, other], D.at[t, other], bs.at[t, i - 1], br.at[t, i - 1], at(b=other))

    def unit(t, k, pair, width):
        src, dst = (t if k == 1 else k), k + 1
        y0, x0 = row_of(pair), H + NX // 2 - width // 2
        u = {}
        for dx in range(-2, width + 2):
            for dy in range(-2, 4):
                if 0 <= dx < width or 0 <= dy < 2:
                    u[dx, dy] = S[src, x0 + dx, y0 + dy]
        stack = jnp.concatenate([u[dx, dy] for dx in range(width) for dy in range(2)], axis=0)
        high = stack.astype(jnp.bfloat16)
        low = (stack - high.astype(jnp.float32)).astype(jnp.bfloat16)
        along = jnp.dot(
            jnp.concatenate([high, low], axis=1), Z[...], preferred_element_type=jnp.float32
        )
        for dx in range(width):
            for dy in range(2):
                one = (u[dx - 1, dy] + u[dx + 1, dy]) + (u[dx, dy - 1] + u[dx, dy + 1])
                two = (u[dx - 2, dy] + u[dx + 2, dy]) + (u[dx, dy - 2] + u[dx, dy + 2])
                at_cell = F * (2 * dx + dy)
                around = (two + along[at_cell : at_cell + F]) - 16.0 * one
                S[dst, x0 + dx, y0 + dy] = V[t, x0 + dx, y0 + dy] * u[dx, dy] + far_w * around
        if width > NX:
            for d, edge in ((0, H - 2), (1, H + NX)):

                @pl.when(jnp.logical_not(x_there[d]))
                def _(edge=edge):
                    for dx in range(2):
                        for dy in range(2):
                            S[dst, edge + dx, y0 + dy] = zero

    def stage(t, j):
        if j == 0:
            for k in range(1, 5):

                def one_pair(pair, carry, k=k):
                    unit(t, k, pair, NX + 4 * (4 - k))
                    return carry

                lax.fori_loop(k, 10 - k, one_pair, 0)
            return

        def some(ks):
            for k in ks:
                unit(t, k, k - j, NX + 4 * (4 - k - max(j - k, 0)))

        if j > 1:
            pl.when(far_there)(lambda: some(range(1, j)))
        some(range(j, 5))

    sub = lax.broadcasted_iota(jnp.int32, (F, NZ), 0)
    sign = jnp.where(sub < F // 2, 1.0, -1.0)

    def combine(s, w):
        even = w[0] + ((s**4 / 24.0) * w[4] - (s**2 / 2.0) * w[2])
        odd_part = s * w[1] - (s**3 / 6.0) * w[3]
        return even + sign * pltpu.roll(odd_part, F // 2, 0)

    def each_of(pair, body):
        y0 = row_of(pair)

        def step(i, carry):
            for dx in range(4):
                for dy in range(2):
                    body(4 * i + dx, y0 - H + dy)
            return carry

        lax.fori_loop(0, NX // 4, step, 0)

    def terms(t, x, y):
        return [S[t, H + x, H + y]] + [S[k, H + x, H + y] for k in range(2, 6)]

    def half_way(x, y):
        w = terms(0, x, y)
        D[1, band, x, y] = density_of(combine(step_length, w))
        S[1, H + x, H + y] = combine(step_length / 2, w)

    def half_row(pair):
        each_of(pair, half_way)
        if pair < 4:
            send_y(1, 1, [pair + 1])
        if pair > 1:
            send_y(1, 0, [6 - pair])
        send_x(1, [pair])

    def take_out(x, y):
        out[pl.ds(x * NY + y, F, stride=NX * NY), :] = combine(step_length / 2, terms(1, x, y))

    def out_row(pair):
        each_of(pair, take_out)

    def to_potential(t):
        def cell(x, y):
            total = (D[t, 0, x, y] + D[t, 1, x, y]) + (D[t, 2, x, y] + D[t, 3, x, y])
            v = ext[pl.ds(x * NY + y, 1), :] - exchange_coef * cube_root(total)
            if t == 1:
                pot[pl.ds(x * NY + y, 1), :] = v
            V[t, H + x, H + y] = v + centre

        own_cells(cell, 4)

    def sum_over_band(t):
        for i in range(1, n_band):
            band_from(t, i).wait_recv()

    U, W = range(1, 5), range(1, 4)

    for i in range(1, n_band):
        band_copy(0, i).start()
    send_y(0, 1, [1, 2])
    send_y(0, 0, U)
    send_x(0, x_pairs(0))
    scope('band0')(sum_over_band)(0)
    scope('pot0')(to_potential)(0)
    send_y(2, 1, W)
    send_y(2, 0, W)
    send_x(2, x_pairs(2))
    send_y(0, 1, [3, 4])
    with jax.named_scope('near0'):
        pass_on(0, 0, U)
        pass_on(2, 0, W)
    with jax.named_scope('x0'):
        await_x(0)
        await_x(2)
    with jax.named_scope('nearrelay0'):
        await_relay(0, 0, W)
        await_relay(2, 0, [1, 2])
    with jax.named_scope('stage00'):
        stage(0, 0)
    with jax.named_scope('half00'):
        half_row(5)
        half_row(4)
    with jax.named_scope('far01'):
        pass_on(0, 1, [1])
    for j in range(1, 5):
        if j < 4:
            with jax.named_scope(f'farU0{j+1}'):
                pass_on(0, 1, [j + 1])
            with jax.named_scope(f'farV0{j}'):
                pass_on(2, 1, [j])
            with jax.named_scope(f'farrelay0{j}'):
                await_relay(0, 1, [j])
                if j > 1:
                    await_relay(2, 1, [j - 1])
        with jax.named_scope(f'stage0{j}'):
            stage(0, j)
        with jax.named_scope(f'half0{j}'):
            half_row(4 - j)

    for i in range(1, n_band):
        band_copy(1, i).start()
    with jax.named_scope('near1'):
        pass_on(1, 0, U)
    scope('band1')(sum_over_band)(1)
    scope('pot1')(to_potential)(1)
    send_y(3, 1, W)
    send_y(3, 0, W)
    send_x(3, x_pairs(3))
    with jax.named_scope('nearV1'):
        pass_on(3, 0, W)
    with jax.named_scope('x1'):
        await_x(1)
        await_x(3)
    with jax.named_scope('nearrelay1'):
        await_relay(1, 0, W)
        await_relay(3, 0, [1, 2])
    with jax.named_scope('stage10'):
        stage(1, 0)
        out_row(5)
        out_row(4)
    with jax.named_scope('farU1'):
        pass_on(1, 1, [4, 3, 2, 1])
    with jax.named_scope('farV1'):
        pass_on(3, 1, W)
    with jax.named_scope('farrelay1'):
        await_relay(1, 1, W)
        await_relay(3, 1, [1, 2])
    with jax.named_scope('stages1'):
        for j in range(1, 5):
            stage(1, j)
            out_row(4 - j)
    with jax.named_scope('drain'):
        for t in range(2):
            for i in range(1, n_band):
                band_copy(t, i).wait_send()
            drain(t)
            drain(t + 2)


def body(orbitals, external):
    rows = NX * NY
    vmem = pl.BlockSpec(memory_space=pltpu.VMEM)
    dma = pltpu.SemaphoreType.DMA
    out, pot = pl.pallas_call(
        kernel,
        out_shape=(
            jax.ShapeDtypeStruct((F * rows, NZ), jnp.float32),
            jax.ShapeDtypeStruct((rows, NZ), jnp.float32),
        ),
        in_specs=[vmem, vmem],
        out_specs=(vmem, vmem),
        scratch_shapes=[
            pltpu.VMEM((6, EX, EY, F, NZ), jnp.float32),
            pltpu.VMEM((2, EX, EY, 1, NZ), jnp.float32),
            pltpu.VMEM((2, 4, NX, NY, 1, NZ), jnp.float32),
            pltpu.VMEM((2 * NZ, NZ), jnp.bfloat16),
            dma((4, 2, 4)),
            dma((4, 2, 4)),
            dma((4, 6, 2)),
            dma((4, 6, 2)),
            dma((4, 2, 3, 2)),
            dma((4, 2, 3, 2)),
            dma((2, 3)),
            dma((2, 3)),
        ],
        compiler_params=pltpu.CompilerParams(
            collective_id=0, has_side_effects=True, vmem_limit_bytes=40 * 1024 * 1024
        ),
        name="etrs",
    )(orbitals.reshape(F * rows, NZ), external.reshape(rows, NZ))
    return out.reshape(orbitals.shape), pot.reshape(external.shape)


def solution(mesh):
    in_specs = (P(None, "band", "gx", "gy", None), P("gx", "gy", None))
    out_specs = (P(None, "band", "gx", "gy", None), P("gx", "gy", None))
    return jax.shard_map(body, mesh=mesh, in_specs=in_specs, out_specs=out_specs, check_vma=False)
```

```python
import functools

import jax
import jax.numpy as jnp
from jax import lax
from jax.experimental import pallas as pl
from jax.experimental.pallas import tpu as pltpu
from jax.sharding import PartitionSpec as P

step_length = 0.15
exchange_coef = 0.7386
centre = 3.75
far_w = 1.0 / 24.0

MESH = pl.DeviceIdType.MESH
F = 8
NX, NY, NZ = 8, 12, 128
H = 8
EX, EY = NX + 2 * H, NY + 2 * H


def cube_root(x):
    safe = jnp.maximum(x, 1e-37)
    y = jnp.exp(jnp.log(safe) * (1.0 / 3.0))
    y = y - (y - safe / (y * y)) * (1.0 / 3.0)
    return jnp.where(x > 1e-37, y, 0.0)


def kernel(orb_in, ext_in, out, pot, S, V, D, Z, orb, ext, ys, yr, xs, xr, rs, rr, bs, br, vs, vr, ins):
    gx, gy, band = lax.axis_index("gx"), lax.axis_index("gy"), lax.axis_index("band")
    n_gx, n_gy, n_band = lax.axis_size("gx"), lax.axis_size("gy"), lax.axis_size("band")
    odd = lax.rem(gy, 2)
    y_right = (odd == 0, odd == 1)
    y_gy = (gy + 1 - 2 * odd, jnp.clip(gy - 1 + 2 * odd, 0, n_gy - 1))
    far_there = (gy > 0) & (gy < n_gy - 1)
    x_gx = (jnp.maximum(gx - 1, 0), jnp.minimum(gx + 1, n_gx - 1))
    x_there = (gx > 0, gx < n_gx - 1)

    def at(x=gx, y=gy, b=band):
        return (x, y, b)

    def when_side(side, more=None):
        if side == 0:
            return pl.when(more) if more is not None else (lambda f: f())
        return pl.when(far_there & more) if more is not None else pl.when(far_there)

    bar = pltpu.get_barrier_semaphore()

    def greet(dev):
        pl.semaphore_signal(bar, inc=1, device_id=dev, device_id_type=MESH)

    count = jnp.int32(n_band)
    pl.when(far_there)(lambda: greet(at(y=y_gy[1])))
    count = count + far_there.astype(jnp.int32)
    for d in range(2):
        pl.when(x_there[d])(lambda d=d: greet(at(x=x_gx[d])))
        count = count + x_there[d].astype(jnp.int32)
    for i in range(1, n_band):
        greet(at(b=lax.rem(band + i, n_band)))
    greet(at(y=y_gy[0]))

    fetch = [pltpu.make_async_copy(a, b, ins.at[i]) for i, (a, b) in enumerate(((orb_in, orb), (ext_in, ext)))]
    for copy in fetch:
        copy.start()

    def density_of(u):
        return jnp.sum(u * u, axis=0, keepdims=True)

    def own_cells(body, unroll):
        def step(i, carry):
            for j in range(unroll):
                body(lax.div(i, NY // unroll), lax.rem(i, NY // unroll) * unroll + j)
            return carry

        lax.fori_loop(0, NX * (NY // unroll), step, 0)

    def take_in(x, y):
        u = orb[pl.ds(y * NX + x, F, stride=NX * NY), :]
        S[0, H + x, H + y] = u
        D[0, band, x, y] = density_of(u)

    off = jnp.abs(lax.broadcasted_iota(jnp.int32, (NZ, NZ), 0) - lax.broadcasted_iota(jnp.int32, (NZ, NZ), 1))
    z_part = jnp.where(off == 1, -16.0, jnp.where(off == 2, 1.0, 0.0)).astype(jnp.bfloat16)
    Z[0:NZ, :] = z_part
    Z[NZ:, :] = z_part

    for copy in fetch:
        copy.wait()
    own_cells(take_in, 4)

    zero = jnp.zeros((F, NZ), jnp.float32)

    def clear_x(x0):
        def step(i, carry):
            for slot in range(5):
                for dx in range(2):
                    S[slot, x0 + dx, i] = zero
            return carry

        lax.fori_loop(0, EY, step, 0)

    def clear_y(y0):
        def step(i, carry):
            for slot in range(5):
                for dy in range(2):
                    S[slot, i, y0 + dy] = zero
            return carry

        lax.fori_loop(0, EX, step, 0)

    pl.when(gx == 0)(lambda: clear_x(H - 2))
    pl.when(gx == n_gx - 1)(lambda: clear_x(H + NX))
    pl.when(gy == 0)(lambda: clear_y(H - 2))
    pl.when(gy == n_gy - 1)(lambda: clear_y(H + NY))

    with jax.named_scope('barrier'):
        pl.semaphore_wait(bar, count)

    def remote(src, dst, s, r, dev):
        return pltpu.make_async_remote_copy(
            src_ref=src, dst_ref=dst, send_sem=s, recv_sem=r, device_id=dev, device_id_type=MESH
        )

    def row_of(pair):
        return jnp.where(odd == 1, H + NY - 2 - 2 * pair, H + 2 * pair)

    def ref_of(e):
        return S.at[e] if e < 2 else V.at[e - 2]

    def reach(e):
        return 4 if e < 2 else 3

    def y_copy(e, side, j):
        buf = ref_of(e)
        src_y = jnp.where(y_right[side], H + NY - 2 * j, H + 2 * (j - 1))
        dst_y = jnp.where(y_right[side], H - 2 * j, H + NY + 2 * (j - 1))
        return remote(
            buf.at[pl.ds(H, NX), pl.ds(src_y, 2)],
            buf.at[pl.ds(H, NX), pl.ds(dst_y, 2)],
            ys.at[e, side, j - 1],
            yr.at[e, side, j - 1],
            at(y=y_gy[side]),
        )

    def x_copy(e, pair, d):
        buf = ref_of(e)
        depth = 2 * reach(e)
        rows = pl.ds(row_of(pair), 2)
        src_x = H if d == 0 else H + NX - depth
        dst_x = H + NX if d == 0 else H - depth
        return remote(
            buf.at[pl.ds(src_x, depth), rows],
            buf.at[pl.ds(dst_x, depth), rows],
            xs.at[e, pair, d],
            xr.at[e, pair, d],
            at(x=x_gx[d]),
        )

    def relay(e, side, j, d):
        buf = ref_of(e)
        depth = 2 * (reach(e) - j)
        src_y = jnp.where(y_right[side], H + NY - 2 * j, H + 2 * (j - 1))
        dst_y = jnp.where(y_right[side], H - 2 * j, H + NY + 2 * (j - 1))
        if side == 0:
            dst_x = H - depth if d == 0 else H + NX
            src_x, dev = dst_x, at(y=y_gy[0])
        else:
            dst_y = src_y = jnp.where(y_right[1], H + NY + 2 * (j - 1), H - 2 * j)
            src_x = H if d == 0 else H + NX - depth
            dst_x = H + NX if d == 0 else H - depth
            dev = at(x=x_gx[d])
        return remote(
            buf.at[pl.ds(src_x, depth), pl.ds(src_y, 2)],
            buf.at[pl.ds(dst_x, depth), pl.ds(dst_y, 2)],
            rs.at[e, side, j - 1, d],
            rr.at[e, side, j - 1, d],
            dev,
        )

    def send_y(e, side, pieces):
        @when_side(side)
        def _():
            for j in pieces:
                y_copy(e, side, j).start()

    def send_x(e, pairs):
        for d in range(2):

            @pl.when(x_there[d])
            def _(d=d):
                for pair in pairs:
                    x_copy(e, pair, d).start()

    def take_far(e, pieces):
        @when_side(1)
        def _():
            for j in pieces:
                y_copy(e, 1, j).wait_recv()
                if j < reach(e):
                    for d in range(2):
                        pl.when(x_there[d])(lambda j=j, d=d: relay(e, 1, j, d).start())

    def spread(j, i):
        part = V.at[0, pl.ds(H, NX), pl.ds(row_of(-j), 2)]
        return remote(part, part, vs.at[j - 1, i - 1], vr.at[j - 1], at(b=lax.rem(band + i, n_band)))

    def take_far_potential(pieces):
        for j in pieces:

            @pl.when(far_there & (band == j - 1))
            def _(j=j):
                y_copy(2, 1, j).wait_recv()
                for i in range(1, n_band):
                    spread(j, i).start()

            @pl.when(far_there & (band != j - 1))
            def _(j=j):
                spread(j, 1).wait_recv()

            if j < 3:
                for d in range(2):
                    when_side(1, x_there[d])(lambda j=j, d=d: relay(2, 1, j, d).start())

    def await_near(e):
        for j in range(1, reach(e) + 1):
            y_copy(e, 0, j).wait_recv()

    def await_relay(e, side, pieces):
        for d in range(2):

            @when_side(side, x_there[d])
            def _(d=d):
                for j in pieces:
                    relay(e, side, j, 1 - d if side else d).wait_recv()

    def await_x(e, pairs):
        for d in range(2):

            @pl.when(x_there[d])
            def _(d=d):
                for pair in pairs:
                    x_copy(e, pair, 1 - d).wait_recv()
                    j = NY // 2 - pair
                    if j < reach(e):
                        relay(e, 0, j, d).start()

    def drain(e):
        for side in range(2):

            for j in range(1, reach(e) + 1):
                if side == 0 or e != 2:
                    when_side(side)(lambda j=j, side=side: y_copy(e, side, j).wait_send())
                else:

                    @pl.when(far_there & (band == j - 1))
                    def _(j=j):
                        y_copy(e, 1, j).wait_send()
                        for i in range(1, n_band):
                            spread(j, i).wait_send()

            for d in range(2):

                @when_side(side, x_there[d])
                def _(side=side, d=d):
                    for j in range(1, reach(e)):
                        relay(e, side, j, d).wait_send()

        for d in range(2):

            @pl.when(x_there[d])
            def _(d=d):
                for pair in range(NY // 2):
                    x_copy(e, pair, d).wait_send()

    def band_rows(t, whose, pair):
        return D.at[t, whose, pl.ds(0, NX), pl.ds(row_of(pair) - H, 2)]

    def band_copy(t, pair, i):
        part = band_rows(t, band, pair)
        return remote(part, part, bs.at[t, pair, i - 1], br.at[t, pair, i - 1], at(b=lax.rem(band + i, n_band)))

    def band_from(t, pair, i):
        other = lax.rem(band + n_band - i, n_band)
        part = band_rows(t, other, pair)
        return remote(part, part, bs.at[t, pair, i - 1], br.at[t, pair, i - 1], at(b=other))

    def send_band(t, pair):
        for i in range(1, n_band):
            band_copy(t, pair, i).start()

    def unit(t, k, pair, width):
        src, dst = (t if k == 1 else k), k + 1
        y0, x0 = row_of(pair), H + NX // 2 - width // 2
        u = {}
        for dx in range(-2, width + 2):
            for dy in range(-2, 4):
                if 0 <= dx < width or 0 <= dy < 2:
                    u[dx, dy] = S[src, x0 + dx, y0 + dy]
        stack = jnp.concatenate([u[dx, dy] for dx in range(width) for dy in range(2)], axis=0)
        high = stack.astype(jnp.bfloat16)
        low = (stack - high.astype(jnp.float32)).astype(jnp.bfloat16)
        along = jnp.dot(
            jnp.concatenate([high, low], axis=1), Z[...], preferred_element_type=jnp.float32
        )
        for dx in range(width):
            for dy in range(2):
                one = (u[dx - 1, dy] + u[dx + 1, dy]) + (u[dx, dy - 1] + u[dx, dy + 1])
                two = (u[dx - 2, dy] + u[dx + 2, dy]) + (u[dx, dy - 2] + u[dx, dy + 2])
                at_cell = F * (2 * dx + dy)
                around = (two + along[at_cell : at_cell + F]) - 16.0 * one
                S[dst, x0 + dx, y0 + dy] = V[t, x0 + dx, y0 + dy] * u[dx, dy] + far_w * around
        if width > NX:
            for d, edge in ((0, H - 2), (1, H + NX)):

                @pl.when(jnp.logical_not(x_there[d]))
                def _(edge=edge):
                    for dx in range(2):
                        for dy in range(2):
                            S[dst, edge + dx, y0 + dy] = zero

    def stage(t, j):
        if j == 0:
            for k in range(1, 5):

                def one_pair(pair, carry, k=k):
                    unit(t, k, pair, NX + 4 * (4 - k))
                    return carry

                lax.fori_loop(k, 10 - k, one_pair, 0)
            return

        def some(ks):
            for k in ks:
                unit(t, k, k - j, NX + 4 * (4 - k - max(j - k, 0)))

        if j > 1:
            pl.when(far_there)(lambda: some(range(1, j)))
        some(range(j, 5))

    sub = lax.broadcasted_iota(jnp.int32, (F, NZ), 0)
    sign = jnp.where(sub < F // 2, 1.0, -1.0)

    def combine(s, w):
        even = w[0] + ((s**4 / 24.0) * w[4] - (s**2 / 2.0) * w[2])
        odd_part = s * w[1] - (s**3 / 6.0) * w[3]
        return even + sign * pltpu.roll(odd_part, F // 2, 0)

    def each_of(pair, body):
        y0 = row_of(pair)

        def step(i, carry):
            for dx in range(4):
                for dy in range(2):
                    body(4 * i + dx, y0 - H + dy)
            return carry

        lax.fori_loop(0, NX // 4, step, 0)

    def terms(t, x, y):
        return [S[t, H + x, H + y]] + [S[k, H + x, H + y] for k in range(2, 6)]

    def half_way(x, y):
        w = terms(0, x, y)
        D[1, band, x, y] = density_of(combine(step_length, w))
        S[1, H + x, H + y] = combine(step_length / 2, w)

    def half_row(pair):
        each_of(pair, half_way)
        send_band(1, pair)
        if 0 < pair < 4:
            send_y(1, 1, [pair + 1])
        if pair > 1:
            send_y(1, 0, [6 - pair])
        send_x(1, [pair])

    def take_out(x, y):
        out[pl.ds(y * NX + x, F, stride=NX * NY), :] = combine(step_length / 2, terms(1, x, y))

    def out_row(pair):
        each_of(pair, take_out)

    def potential_row(t, pair):
        for i in range(1, n_band):
            band_from(t, pair, i).wait_recv()

        def cell(x, y):
            total = (D[t, 0, x, y] + D[t, 1, x, y]) + (D[t, 2, x, y] + D[t, 3, x, y])
            v = ext[pl.ds(y * NX + x, 1), :] - exchange_coef * cube_root(total)
            if t == 1:
                pot[pl.ds(y * NX + x, 1), :] = v
            V[t, H + x, H + y] = v + centre

        each_of(pair, cell)
        if pair < 3:
            mine = far_there & (band == pair) if t == 0 else far_there
            pl.when(mine)(lambda: y_copy(t + 2, 1, pair + 1).start())
        else:
            send_y(t + 2, 0, [6 - pair])
        send_x(t + 2, [pair])

    scope = jax.named_scope
    rows = range(NY // 2)

    send_y(0, 1, [1, 2])
    for pair in rows:
        send_band(0, pair)
    send_y(0, 0, range(1, 5))
    send_x(0, rows)
    with scope('pot0'):
        for pair in rows:
            potential_row(0, pair)
    send_y(0, 1, [3, 4])
    with scope('far01'):
        take_far(0, [1])
    with scope('x0'):
        await_x(0, rows)
        await_x(2, rows)
    with scope('near0'):
        await_near(0)
        await_near(2)
        await_relay(0, 0, [1, 2, 3])
        await_relay(2, 0, [1, 2])
    with scope('stage00'):
        stage(0, 0)
    with scope('half00'):
        half_row(5)
        half_row(4)
    for j in range(1, 5):
        with scope(f'far0{j}'):
            if j < 4:
                take_far(0, [j + 1])
                take_far_potential([j])
        with scope(f'farrelay0{j}'):
            if j < 4:
                await_relay(0, 1, [j])
                if j > 1:
                    await_relay(2, 1, [j - 1])
        with scope(f'stage0{j}'):
            stage(0, j)
            half_row(4 - j)
        with scope(f'pot1{j}'):
            if j == 1:
                potential_row(1, 5)
                potential_row(1, 4)
            else:
                potential_row(1, 5 - j)

    with scope('pot15'):
        potential_row(1, 0)
    send_y(1, 1, [1])
    with scope('far1a'):
        take_far(1, [4, 3, 2])
    with scope('x1'):
        await_x(1, rows)
        await_x(3, rows)
    with scope('near1'):
        await_near(1)
        await_near(3)
        await_relay(1, 0, [1, 2, 3])
        await_relay(3, 0, [1, 2])
    with scope('stage10'):
        stage(1, 0)
        out_row(5)
        out_row(4)
    with scope('farV1'):
        take_far(3, [3, 2, 1])
        take_far(1, [1])
    with scope('farrelay1'):
        await_relay(1, 1, [1, 2, 3])
    with scope('stage11'):
        stage(1, 1)
        out_row(3)
    with scope('farrelayV1'):
        await_relay(3, 1, [1, 2])
    with scope('stages1'):
        for j in range(2, 5):
            stage(1, j)
            out_row(4 - j)
    with scope('drain'):
        for t in range(2):
            for pair in rows:
                for i in range(1, n_band):
                    band_copy(t, pair, i).wait_send()
            drain(t)
            drain(t + 2)


def body(orbitals, external):
    rows = NX * NY
    vmem = pl.BlockSpec(memory_space=pltpu.VMEM)
    dma = pltpu.SemaphoreType.DMA
    out, pot = pl.pallas_call(
        kernel,
        out_shape=(
            jax.ShapeDtypeStruct((F * rows, NZ), jnp.float32),
            jax.ShapeDtypeStruct((rows, NZ), jnp.float32),
        ),
        in_specs=[pl.BlockSpec(memory_space=pltpu.HBM)] * 2,
        out_specs=(vmem, vmem),
        scratch_shapes=[
            pltpu.VMEM((6, EX, EY, F, NZ), jnp.float32),
            pltpu.VMEM((2, EX, EY, 1, NZ), jnp.float32),
            pltpu.VMEM((2, 4, NX, NY, 1, NZ), jnp.float32),
            pltpu.VMEM((2 * NZ, NZ), jnp.bfloat16),
            pltpu.VMEM((F * rows, NZ), jnp.float32),
            pltpu.VMEM((rows, NZ), jnp.float32),
            dma((4, 2, 4)),
            dma((4, 2, 4)),
            dma((4, 6, 2)),
            dma((4, 6, 2)),
            dma((4, 2, 3, 2)),
            dma((4, 2, 3, 2)),
            dma((2, 6, 3)),
            dma((2, 6, 3)),
            dma((3, 3)),
            dma((3,)),
            dma((2,)),
        ],
        compiler_params=pltpu.CompilerParams(
            collective_id=0, has_side_effects=True, vmem_limit_bytes=40 * 1024 * 1024
        ),
        name="etrs",
    )(
        pltpu.with_memory_space_constraint(orbitals.transpose(0, 1, 3, 2, 4).reshape(F * rows, NZ), pltpu.HBM),
        pltpu.with_memory_space_constraint(external.transpose(1, 0, 2).reshape(rows, NZ), pltpu.HBM),
    )
    out = out.reshape(2, F // 2, NY, NX, NZ).transpose(0, 1, 3, 2, 4)
    return out, pot.reshape(NY, NX, NZ).transpose(1, 0, 2)


def solution(mesh):
    in_specs = (P(None, "band", "gx", "gy", None), P("gx", "gy", None))
    out_specs = (P(None, "band", "gx", "gy", None), P("gx", "gy", None))
    return jax.shard_map(body, mesh=mesh, in_specs=in_specs, out_specs=out_specs, check_vma=False)
```

```python
import functools

import jax
import jax.numpy as jnp
from jax import lax
from jax.experimental import pallas as pl
from jax.experimental.pallas import tpu as pltpu
from jax.sharding import PartitionSpec as P

step_length = 0.15
exchange_coef = 0.7386
centre = 3.75
far_w = 1.0 / 24.0

MESH = pl.DeviceIdType.MESH
F = 8
NX, NY, NZ = 8, 12, 128
H = 8
M = 0
HY = H + 2 * M
EX, EY = NX + 2 * H, NY + 2 * HY


def cube_root(x):
    safe = jnp.maximum(x, 1e-37)
    y = jnp.exp(jnp.log(safe) * (1.0 / 3.0))
    y = y - (y - safe / (y * y)) * (1.0 / 3.0)
    return jnp.where(x > 1e-37, y, 0.0)


def kernel(orb_in, ext_in, out, pot, S, V, D, Z, orb, ext, ys, yr, xs, xr, rs, rr, bs, br, vs, vr, ins):
    gx, gy, band = lax.axis_index("gx"), lax.axis_index("gy"), lax.axis_index("band")
    n_gx, n_gy, n_band = lax.axis_size("gx"), lax.axis_size("gy"), lax.axis_size("band")
    odd = lax.rem(gy, 2)
    y_right = (odd == 0, odd == 1)
    y_gy = (gy + 1 - 2 * odd, jnp.clip(gy - 1 + 2 * odd, 0, n_gy - 1))
    far_there = (gy > 0) & (gy < n_gy - 1)
    x_gx = (jnp.maximum(gx - 1, 0), jnp.minimum(gx + 1, n_gx - 1))
    x_there = (gx > 0, gx < n_gx - 1)

    def at(x=gx, y=gy, b=band):
        return (x, y, b)

    def when_side(side, more=None):
        if side == 0:
            return pl.when(more) if more is not None else (lambda f: f())
        return pl.when(far_there & more) if more is not None else pl.when(far_there)

    bar = pltpu.get_barrier_semaphore()

    def greet(dev):
        pl.semaphore_signal(bar, inc=1, device_id=dev, device_id_type=MESH)

    count = jnp.int32(n_band)
    pl.when(far_there)(lambda: greet(at(y=y_gy[1])))
    count = count + far_there.astype(jnp.int32)
    for d in range(2):
        pl.when(x_there[d])(lambda d=d: greet(at(x=x_gx[d])))
        count = count + x_there[d].astype(jnp.int32)
    for i in range(1, n_band):
        greet(at(b=lax.rem(band + i, n_band)))
    greet(at(y=y_gy[0]))

    fetch = [pltpu.make_async_copy(a, b, ins.at[i]) for i, (a, b) in enumerate(((orb_in, orb), (ext_in, ext)))]
    for copy in fetch:
        copy.start()

    def density_of(u):
        return jnp.sum(u * u, axis=0, keepdims=True)

    def own_cells(body, unroll):
        def step(i, carry):
            for j in range(unroll):
                body(lax.div(i, NY // unroll), lax.rem(i, NY // unroll) * unroll + j)
            return carry

        lax.fori_loop(0, NX * (NY // unroll), step, 0)

    def take_in(x, y):
        u = orb[pl.ds(y * NX + x, F, stride=NX * NY), :]
        S[0, H + x, HY + y] = u
        D[0, band, x, y] = density_of(u)

    off = jnp.abs(lax.broadcasted_iota(jnp.int32, (NZ, NZ), 0) - lax.broadcasted_iota(jnp.int32, (NZ, NZ), 1))
    z_part = jnp.where(off == 1, -16.0, jnp.where(off == 2, 1.0, 0.0)).astype(jnp.bfloat16)
    Z[0:NZ, :] = z_part
    Z[NZ:, :] = z_part

    for copy in fetch:
        copy.wait()
    own_cells(take_in, 4)

    zero = jnp.zeros((F, NZ), jnp.float32)

    def clear_x(x0):
        def step(i, carry):
            for slot in range(5):
                for dx in range(2):
                    S[slot, x0 + dx, i] = zero
            return carry

        lax.fori_loop(0, EY, step, 0)

    def clear_y(y0):
        def step(i, carry):
            for slot in range(5):
                for dy in range(2):
                    S[slot, i, y0 + dy] = zero
            return carry

        lax.fori_loop(0, EX, step, 0)

    pl.when(gx == 0)(lambda: clear_x(H - 2))
    pl.when(gx == n_gx - 1)(lambda: clear_x(H + NX))
    pl.when(gy == 0)(lambda: clear_y(HY - 2))
    pl.when(gy == n_gy - 1)(lambda: clear_y(HY + NY))

    with jax.named_scope('barrier'):
        pl.semaphore_wait(bar, count)

    def remote(src, dst, s, r, dev):
        return pltpu.make_async_remote_copy(
            src_ref=src, dst_ref=dst, send_sem=s, recv_sem=r, device_id=dev, device_id_type=MESH
        )

    def row_of(pair):
        return jnp.where(odd == 1, HY + NY - 2 - 2 * pair, HY + 2 * pair)

    def ref_of(e):
        return S.at[e] if e < 2 else V.at[e - 2]

    def reach(e):
        return 4 if e < 2 else 3

    def pieces_of(e, side):
        more = M if side == 1 and e in (0, 2) else 0
        return range(M + 1 if side == 1 and e == 1 else 1, reach(e) + more + 1)

    def depth_of(e, side, j):
        more = M if side == 1 and e in (0, 2) else 0
        return 2 * min(reach(e), reach(e) + more - j)

    def relays_of(e, side):
        return [j for j in range(1, 4 + M) if depth_of(e, side, j) > 0]

    def y_copy(e, side, j):
        buf = ref_of(e)
        src_y = jnp.where(y_right[side], HY + NY - 2 * j, HY + 2 * (j - 1))
        dst_y = jnp.where(y_right[side], HY - 2 * j, HY + NY + 2 * (j - 1))
        return remote(
            buf.at[pl.ds(H, NX), pl.ds(src_y, 2)],
            buf.at[pl.ds(H, NX), pl.ds(dst_y, 2)],
            ys.at[e, side, j - 1],
            yr.at[e, side, j - 1],
            at(y=y_gy[side]),
        )

    def x_copy(e, pair, d):
        buf = ref_of(e)
        depth = 2 * reach(e)
        rows = pl.ds(row_of(pair), 2)
        src_x = H if d == 0 else H + NX - depth
        dst_x = H + NX if d == 0 else H - depth
        return remote(
            buf.at[pl.ds(src_x, depth), rows],
            buf.at[pl.ds(dst_x, depth), rows],
            xs.at[e, pair, d],
            xr.at[e, pair, d],
            at(x=x_gx[d]),
        )

    def relay(e, side, j, d):
        buf = ref_of(e)
        depth = depth_of(e, side, j)
        src_y = jnp.where(y_right[side], HY + NY - 2 * j, HY + 2 * (j - 1))
        dst_y = jnp.where(y_right[side], HY - 2 * j, HY + NY + 2 * (j - 1))
        if side == 0:
            dst_x = H - depth if d == 0 else H + NX
            src_x, dev = dst_x, at(y=y_gy[0])
        else:
            dst_y = src_y = jnp.where(y_right[1], HY + NY + 2 * (j - 1), HY - 2 * j)
            src_x = H if d == 0 else H + NX - depth
            dst_x = H + NX if d == 0 else H - depth
            dev = at(x=x_gx[d])
        return remote(
            buf.at[pl.ds(src_x, depth), pl.ds(src_y, 2)],
            buf.at[pl.ds(dst_x, depth), pl.ds(dst_y, 2)],
            rs.at[e, side, j - 1, d],
            rr.at[e, side, j - 1, d],
            dev,
        )

    def send_y(e, side, pieces):
        @when_side(side)
        def _():
            for j in pieces:
                y_copy(e, side, j).start()

    def send_x(e, pairs):
        for d in range(2):

            @pl.when(x_there[d])
            def _(d=d):
                for pair in pairs:
                    x_copy(e, pair, d).start()

    def take_far(e, pieces):
        @when_side(1)
        def _():
            for j in pieces:
                y_copy(e, 1, j).wait_recv()
                if depth_of(e, 1, j) > 0:
                    for d in range(2):
                        pl.when(x_there[d])(lambda j=j, d=d: relay(e, 1, j, d).start())

    def spread(j, i):
        part = V.at[0, pl.ds(H, NX), pl.ds(row_of(-j), 2)]
        return remote(part, part, vs.at[j - 1, i - 1], vr.at[j - 1], at(b=lax.rem(band + i, n_band)))

    def take_far_potential(pieces):
        for j in pieces:

            @pl.when(far_there & (band == (j - 1) % 4))
            def _(j=j):
                y_copy(2, 1, j).wait_recv()
                for i in range(1, n_band):
                    spread(j, i).start()

            @pl.when(far_there & (band != (j - 1) % 4))
            def _(j=j):
                spread(j, 1).wait_recv()

            if depth_of(2, 1, j) > 0:
                for d in range(2):
                    when_side(1, x_there[d])(lambda j=j, d=d: relay(2, 1, j, d).start())

    def await_near(e):
        for j in range(1, reach(e) + 1):
            y_copy(e, 0, j).wait_recv()

    def await_relay(e, side, pieces):
        for d in range(2):

            @when_side(side, x_there[d])
            def _(d=d):
                for j in pieces:
                    relay(e, side, j, 1 - d if side else d).wait_recv()

    def await_x(e, pairs):
        for d in range(2):

            @pl.when(x_there[d])
            def _(d=d):
                for pair in pairs:
                    x_copy(e, pair, 1 - d).wait_recv()
                    j = NY // 2 - pair
                    if j < reach(e):
                        relay(e, 0, j, d).start()

    def drain(e):
        for side in range(2):
            for j in pieces_of(e, side):
                if side == 0 or e != 2:
                    when_side(side)(lambda j=j, side=side: y_copy(e, side, j).wait_send())
                else:

                    @pl.when(far_there & (band == (j - 1) % 4))
                    def _(j=j):
                        y_copy(e, 1, j).wait_send()
                        for i in range(1, n_band):
                            spread(j, i).wait_send()

            for d in range(2):

                @when_side(side, x_there[d])
                def _(side=side, d=d):
                    for j in relays_of(e, side):
                        relay(e, side, j, d).wait_send()

        for d in range(2):

            @pl.when(x_there[d])
            def _(d=d):
                for pair in range(NY // 2):
                    x_copy(e, pair, d).wait_send()

    def band_rows(t, whose, pair):
        return D.at[t, whose, pl.ds(0, NX), pl.ds(row_of(pair) - HY, 2)]

    def band_copy(t, pair, i):
        part = band_rows(t, band, pair)
        return remote(part, part, bs.at[t, pair, i - 1], br.at[t, pair, i - 1], at(b=lax.rem(band + i, n_band)))

    def band_from(t, pair, i):
        other = lax.rem(band + n_band - i, n_band)
        part = band_rows(t, other, pair)
        return remote(part, part, bs.at[t, pair, i - 1], br.at[t, pair, i - 1], at(b=other))

    def send_band(t, pair):
        for i in range(1, n_band):
            band_copy(t, pair, i).start()

    def unit(t, k, pair, width):
        src, dst = (t if k == 1 else k), k + 1
        y0, x0 = row_of(pair), H + NX // 2 - width // 2
        u = {}
        for dx in range(-2, width + 2):
            for dy in range(-2, 4):
                if 0 <= dx < width or 0 <= dy < 2:
                    u[dx, dy] = S[src, x0 + dx, y0 + dy]
        stack = jnp.concatenate([u[dx, dy] for dx in range(width) for dy in range(2)], axis=0)
        high = stack.astype(jnp.bfloat16)
        low = (stack - high.astype(jnp.float32)).astype(jnp.bfloat16)
        along = jnp.dot(
            jnp.concatenate([high, low], axis=1), Z[...], preferred_element_type=jnp.float32
        )
        for dx in range(width):
            for dy in range(2):
                one = (u[dx - 1, dy] + u[dx + 1, dy]) + (u[dx, dy - 1] + u[dx, dy + 1])
                two = (u[dx - 2, dy] + u[dx + 2, dy]) + (u[dx, dy - 2] + u[dx, dy + 2])
                at_cell = F * (2 * dx + dy)
                around = (two + along[at_cell : at_cell + F]) - 16.0 * one
                S[dst, x0 + dx, y0 + dy] = V[t, x0 + dx, y0 + dy] * u[dx, dy] + far_w * around
        if width > NX:
            for d, edge in ((0, H - 2), (1, H + NX)):

                @pl.when(jnp.logical_not(x_there[d]))
                def _(edge=edge):
                    for dx in range(2):
                        for dy in range(2):
                            S[dst, edge + dx, y0 + dy] = zero

    def stage(t, j, after=False):
        if after:
            for k in range(1, 5):
                unit(t, k, k, NX + 4 * (4 - k))
            return
        if j < 1:
            for k in range(1, 5):

                def one_pair(pair, carry, k=k):
                    unit(t, k, pair, NX + 4 * (4 - k))
                    return carry

                lax.fori_loop(k - j, 10 - k, one_pair, 0)
            return

        def some(ks, j=j):
            for k in ks:
                unit(t, k, k - j, NX + 4 * (4 - k - max(j - k - (0 if t else M), 0)))

        if j > 1:
            pl.when(far_there)(lambda: some(range(1, min(j, 5))))
        some(range(j, 5))

    sub = lax.broadcasted_iota(jnp.int32, (F, NZ), 0)
    sign = jnp.where(sub < F // 2, 1.0, -1.0)

    def combine(s, w):
        even = w[0] + ((s**4 / 24.0) * w[4] - (s**2 / 2.0) * w[2])
        odd_part = s * w[1] - (s**3 / 6.0) * w[3]
        return even + sign * pltpu.roll(odd_part, F // 2, 0)

    def each_of(pair, body):
        y0 = row_of(pair)

        def step(i, carry):
            for dx in range(4):
                for dy in range(2):
                    body(4 * i + dx, y0 - HY + dy)
            return carry

        lax.fori_loop(0, NX // 4, step, 0)

    def terms(t, x, y):
        return [S[t, H + x, HY + y]] + [S[k, H + x, HY + y] for k in range(2, 6)]

    def half_way(x, y):
        w = terms(0, x, y)
        D[1, band, x, y] = density_of(combine(step_length, w))
        S[1, H + x, HY + y] = combine(step_length / 2, w)

    def half_way_only(x, y):
        S[1, H + x, HY + y] = combine(step_length / 2, terms(0, x, y))

    def half_halo_row(pair):
        @pl.when(far_there)
        def _():
            each_of(pair, half_way_only)
            for d in range(2):
                pl.when(x_there[d])(lambda d=d: relay(1, 1, -pair, d).start())

    def half_row(pair):
        each_of(pair, half_way)
        send_band(1, pair)
        if M <= pair < 4:
            send_y(1, 1, [pair + 1])
        if pair > 1:
            send_y(1, 0, [6 - pair])
        send_x(1, [pair])

    def take_out(x, y):
        out[pl.ds(y * NX + x, F, stride=NX * NY), :] = combine(step_length / 2, terms(1, x, y))

    def out_row(pair):
        each_of(pair, take_out)

    def potential_row(t, pair):
        for i in range(1, n_band):
            band_from(t, pair, i).wait_recv()

        def cell(x, y):
            total = (D[t, 0, x, y] + D[t, 1, x, y]) + (D[t, 2, x, y] + D[t, 3, x, y])
            v = ext[pl.ds(y * NX + x, 1), :] - exchange_coef * cube_root(total)
            if t == 1:
                pot[pl.ds(y * NX + x, 1), :] = v
            V[t, H + x, HY + y] = v + centre

        each_of(pair, cell)
        if pair + 1 in pieces_of(t + 2, 1):
            mine = far_there & (band == pair % 4) if t == 0 else far_there
            pl.when(mine)(lambda: y_copy(t + 2, 1, pair + 1).start())
        if pair > 2:
            send_y(t + 2, 0, [6 - pair])
        send_x(t + 2, [pair])

    scope = jax.named_scope
    rows = range(NY // 2)

    send_y(0, 1, [1, 2])
    for pair in rows:
        send_band(0, pair)
    send_y(0, 0, range(1, 5))
    send_x(0, rows)
    with scope('pot0'):
        for pair in rows:
            potential_row(0, pair)
    send_y(0, 1, range(3, 5 + M))
    with scope('far01'):
        take_far(0, [1])
    with scope('x0'):
        await_x(0, rows)
        await_x(2, rows)
    with scope('near0'):
        await_near(0)
        await_near(2)
        await_relay(0, 0, relays_of(0, 0))
        await_relay(2, 0, relays_of(2, 0))
    with scope('far02'):
        take_far(0, [2])
    with scope('stage00'):
        stage(0, 0)
    with scope('half00'):
        half_row(5)
        half_row(4)
    for j in range(1, 5 + M):
        with scope(f'far0{j}'):
            if j in relays_of(0, 1):
                if j > 1 and j + 1 in relays_of(0, 1):
                    take_far(0, [j + 1])
            else:
                take_far(0, [j])
            if j in pieces_of(2, 1):
                take_far_potential([j])
        with scope(f'farrelay0{j}'):
            if j in relays_of(0, 1):
                await_relay(0, 1, [j])
            if j - 1 in relays_of(2, 1):
                await_relay(2, 1, [j - 1])
        with scope(f'stage0{j}'):
            stage(0, j)
            if j < 5:
                half_row(4 - j)
            else:
                half_halo_row(4 - j)
        with scope(f'pot1{j}'):
            if j == 1:
                potential_row(1, 5)
                potential_row(1, 4)
            elif j < 5:
                potential_row(1, 5 - j)
            if j == 4:
                potential_row(1, 0)

    with scope('far1a'):
        take_far(1, range(4, max(M, 1), -1))
    with scope('near1'):
        await_x(1, [5, 4, 3, 2])
        await_x(3, [5, 4, 3, 2])
        await_near(1)
        await_near(3)
        await_x(1, [1])
        await_x(3, [1])
        await_relay(1, 0, relays_of(1, 0))
        await_relay(3, 0, relays_of(3, 0))
    with scope('stage1m'):
        stage(1, -1)
        out_row(5)
    with scope('x1'):
        await_x(1, [0])
    with scope('farV1'):
        take_far(3, [3, 2, 1])
        take_far(1, [1])
    with scope('stage10'):
        stage(1, 0, after=True)
        out_row(4)
    with scope('farrelay1'):
        await_x(3, [0])
        await_relay(1, 1, relays_of(1, 1))
    with scope('stage11'):
        stage(1, 1)
        out_row(3)
    with scope('farrelayV1'):
        await_relay(3, 1, relays_of(3, 1))
    with scope('stages1'):
        for j in range(2, 5):
            stage(1, j)
            out_row(4 - j)
    with scope('drain'):
        for t in range(2):
            for pair in rows:
                for i in range(1, n_band):
                    band_copy(t, pair, i).wait_send()
            drain(t)
            drain(t + 2)


def body(orbitals, external):
    rows = NX * NY
    vmem = pl.BlockSpec(memory_space=pltpu.VMEM)
    dma = pltpu.SemaphoreType.DMA
    out, pot = pl.pallas_call(
        kernel,
        out_shape=(
            jax.ShapeDtypeStruct((F * rows, NZ), jnp.float32),
            jax.ShapeDtypeStruct((rows, NZ), jnp.float32),
        ),
        in_specs=[pl.BlockSpec(memory_space=pltpu.HBM)] * 2,
        out_specs=(vmem, vmem),
        scratch_shapes=[
            pltpu.VMEM((6, EX, EY, F, NZ), jnp.float32),
            pltpu.VMEM((2, EX, EY, 1, NZ), jnp.float32),
            pltpu.VMEM((2, 4, NX, NY, 1, NZ), jnp.float32),
            pltpu.VMEM((2 * NZ, NZ), jnp.bfloat16),
            pltpu.VMEM((F * rows, NZ), jnp.float32),
            pltpu.VMEM((rows, NZ), jnp.float32),
            dma((4, 2, 4 + M)),
            dma((4, 2, 4 + M)),
            dma((4, 6, 2)),
            dma((4, 6, 2)),
            dma((4, 2, 3 + M, 2)),
            dma((4, 2, 3 + M, 2)),
            dma((2, 6, 3)),
            dma((2, 6, 3)),
            dma((3 + M, 3)),
            dma((3 + M,)),
            dma((2,)),
        ],
        compiler_params=pltpu.CompilerParams(
            collective_id=0, has_side_effects=True, vmem_limit_bytes=40 * 1024 * 1024
        ),
        name="etrs",
    )(
        pltpu.with_memory_space_constraint(orbitals.transpose(0, 1, 3, 2, 4).reshape(F * rows, NZ), pltpu.HBM),
        pltpu.with_memory_space_constraint(external.transpose(1, 0, 2).reshape(rows, NZ), pltpu.HBM),
    )
    out = out.reshape(2, F // 2, NY, NX, NZ).transpose(0, 1, 3, 2, 4)
    return out, pot.reshape(NY, NX, NZ).transpose(1, 0, 2)


def solution(mesh):
    in_specs = (P(None, "band", "gx", "gy", None), P("gx", "gy", None))
    out_specs = (P(None, "band", "gx", "gy", None), P("gx", "gy", None))
    return jax.shard_map(body, mesh=mesh, in_specs=in_specs, out_specs=out_specs, check_vma=False)
```

```python
import functools

import jax
import jax.numpy as jnp
from jax import lax
from jax.experimental import pallas as pl
from jax.experimental.pallas import tpu as pltpu
from jax.sharding import PartitionSpec as P

step_length = 0.15
exchange_coef = 0.7386
centre = 3.75
far_w = 1.0 / 24.0

MESH = pl.DeviceIdType.MESH
F = 8
NX, NY, NZ = 8, 12, 128
H = 8
M = 0
HY = H + 2 * M
EX, EY = NX + 2 * H, NY + 2 * HY


def cube_root(x):
    safe = jnp.maximum(x, 1e-37)
    y = jnp.exp(jnp.log(safe) * (1.0 / 3.0))
    y = y - (y - safe / (y * y)) * (1.0 / 3.0)
    return jnp.where(x > 1e-37, y, 0.0)


def kernel(orb_in, ext_in, out, pot, S, V, D, Z, orb, ext, ys, yr, xs, xr, rs, rr, bs, br, vs, vr, ins):
    gx, gy, band = lax.axis_index("gx"), lax.axis_index("gy"), lax.axis_index("band")
    n_gx, n_gy, n_band = lax.axis_size("gx"), lax.axis_size("gy"), lax.axis_size("band")
    odd = lax.rem(gy, 2)
    y_right = (odd == 0, odd == 1)
    y_gy = (gy + 1 - 2 * odd, jnp.clip(gy - 1 + 2 * odd, 0, n_gy - 1))
    far_there = (gy > 0) & (gy < n_gy - 1)
    x_gx = (jnp.maximum(gx - 1, 0), jnp.minimum(gx + 1, n_gx - 1))
    x_there = (gx > 0, gx < n_gx - 1)

    def at(x=gx, y=gy, b=band):
        return (x, y, b)

    def when_side(side, more=None):
        if side == 0:
            return pl.when(more) if more is not None else (lambda f: f())
        return pl.when(far_there & more) if more is not None else pl.when(far_there)

    bar = pltpu.get_barrier_semaphore()

    def greet(dev):
        pl.semaphore_signal(bar, inc=1, device_id=dev, device_id_type=MESH)

    count = jnp.int32(n_band)
    pl.when(far_there)(lambda: greet(at(y=y_gy[1])))
    count = count + far_there.astype(jnp.int32)
    for d in range(2):
        pl.when(x_there[d])(lambda d=d: greet(at(x=x_gx[d])))
        count = count + x_there[d].astype(jnp.int32)
    for i in range(1, n_band):
        greet(at(b=lax.rem(band + i, n_band)))
    greet(at(y=y_gy[0]))

    fetch = [pltpu.make_async_copy(a, b, ins.at[i]) for i, (a, b) in enumerate(((orb_in, orb), (ext_in, ext)))]
    for copy in fetch:
        copy.start()

    def density_of(u):
        return jnp.sum(u * u, axis=0, keepdims=True)

    def own_cells(body, unroll):
        def step(i, carry):
            for j in range(unroll):
                body(lax.div(i, NY // unroll), lax.rem(i, NY // unroll) * unroll + j)
            return carry

        lax.fori_loop(0, NX * (NY // unroll), step, 0)

    def take_in(x, y):
        u = orb[pl.ds(y * NX + x, F, stride=NX * NY), :]
        S[0, H + x, HY + y] = u
        D[0, band, x, y] = density_of(u)

    off = jnp.abs(lax.broadcasted_iota(jnp.int32, (NZ, NZ), 0) - lax.broadcasted_iota(jnp.int32, (NZ, NZ), 1))
    z_part = jnp.where(off == 1, -16.0, jnp.where(off == 2, 1.0, 0.0)).astype(jnp.bfloat16)
    Z[0:NZ, :] = z_part
    Z[NZ:, :] = z_part

    for copy in fetch:
        copy.wait()
    own_cells(take_in, 4)

    zero = jnp.zeros((F, NZ), jnp.float32)

    def clear_x(x0):
        def step(i, carry):
            for slot in range(5):
                for dx in range(2):
                    S[slot, x0 + dx, i] = zero
            return carry

        lax.fori_loop(0, EY, step, 0)

    def clear_y(y0):
        def step(i, carry):
            for slot in range(5):
                for dy in range(2):
                    S[slot, i, y0 + dy] = zero
            return carry

        lax.fori_loop(0, EX, step, 0)

    pl.when(gx == 0)(lambda: clear_x(H - 2))
    pl.when(gx == n_gx - 1)(lambda: clear_x(H + NX))
    pl.when(gy == 0)(lambda: clear_y(HY - 2))
    pl.when(gy == n_gy - 1)(lambda: clear_y(HY + NY))

    with jax.named_scope('barrier'):
        pl.semaphore_wait(bar, count)

    def remote(src, dst, s, r, dev):
        return pltpu.make_async_remote_copy(
            src_ref=src, dst_ref=dst, send_sem=s, recv_sem=r, device_id=dev, device_id_type=MESH
        )

    def row_of(pair):
        return jnp.where(odd == 1, HY + NY - 2 - 2 * pair, HY + 2 * pair)

    def ref_of(e):
        return S.at[e] if e < 2 else V.at[e - 2]

    def reach(e):
        return 4 if e < 2 else 3

    def pieces_of(e, side):
        more = M if side == 1 and e in (0, 2) else 0
        return range(M + 1 if side == 1 and e == 1 else 1, reach(e) + more + 1)

    def depth_of(e, side, j):
        more = M if side == 1 and e in (0, 2) else 0
        return 2 * min(reach(e), reach(e) + more - j)

    def relays_of(e, side):
        return [j for j in range(1, 4 + M) if depth_of(e, side, j) > 0]

    def y_copy(e, side, j):
        buf = ref_of(e)
        src_y = jnp.where(y_right[side], HY + NY - 2 * j, HY + 2 * (j - 1))
        dst_y = jnp.where(y_right[side], HY - 2 * j, HY + NY + 2 * (j - 1))
        return remote(
            buf.at[pl.ds(H, NX), pl.ds(src_y, 2)],
            buf.at[pl.ds(H, NX), pl.ds(dst_y, 2)],
            ys.at[e, side, j - 1],
            yr.at[e, side, j - 1],
            at(y=y_gy[side]),
        )

    def x_copy(e, pair, d):
        buf = ref_of(e)
        depth = 2 * reach(e)
        rows = pl.ds(row_of(pair), 2)
        src_x = H if d == 0 else H + NX - depth
        dst_x = H + NX if d == 0 else H - depth
        return remote(
            buf.at[pl.ds(src_x, depth), rows],
            buf.at[pl.ds(dst_x, depth), rows],
            xs.at[e, pair, d],
            xr.at[e, pair, d],
            at(x=x_gx[d]),
        )

    def relay(e, side, j, d):
        buf = ref_of(e)
        depth = depth_of(e, side, j)
        src_y = jnp.where(y_right[side], HY + NY - 2 * j, HY + 2 * (j - 1))
        dst_y = jnp.where(y_right[side], HY - 2 * j, HY + NY + 2 * (j - 1))
        if side == 0:
            dst_x = H - depth if d == 0 else H + NX
            src_x, dev = dst_x, at(y=y_gy[0])
        else:
            dst_y = src_y = jnp.where(y_right[1], HY + NY + 2 * (j - 1), HY - 2 * j)
            src_x = H if d == 0 else H + NX - depth
            dst_x = H + NX if d == 0 else H - depth
            dev = at(x=x_gx[d])
        return remote(
            buf.at[pl.ds(src_x, depth), pl.ds(src_y, 2)],
            buf.at[pl.ds(dst_x, depth), pl.ds(dst_y, 2)],
            rs.at[e, side, j - 1, d],
            rr.at[e, side, j - 1, d],
            dev,
        )

    def send_y(e, side, pieces):
        @when_side(side)
        def _():
            for j in pieces:
                y_copy(e, side, j).start()

    def send_x(e, pairs):
        for d in range(2):

            @pl.when(x_there[d])
            def _(d=d):
                for pair in pairs:
                    x_copy(e, pair, d).start()

    def take_far(e, pieces):
        @when_side(1)
        def _():
            for j in pieces:
                y_copy(e, 1, j).wait_recv()
                if depth_of(e, 1, j) > 0:
                    for d in range(2):
                        pl.when(x_there[d])(lambda j=j, d=d: relay(e, 1, j, d).start())

    def spread(j, i):
        part = V.at[0, pl.ds(H, NX), pl.ds(row_of(-j), 2)]
        return remote(part, part, vs.at[j - 1, i - 1], vr.at[j - 1], at(b=lax.rem(band + i, n_band)))

    def take_far_potential(pieces):
        for j in pieces:

            @pl.when(far_there & (band == (j - 1) % 4))
            def _(j=j):
                y_copy(2, 1, j).wait_recv()
                for i in range(1, n_band):
                    spread(j, i).start()

            @pl.when(far_there & (band != (j - 1) % 4))
            def _(j=j):
                spread(j, 1).wait_recv()

            if depth_of(2, 1, j) > 0:
                for d in range(2):
                    when_side(1, x_there[d])(lambda j=j, d=d: relay(2, 1, j, d).start())

    def await_near(e):
        for j in range(1, reach(e) + 1):
            y_copy(e, 0, j).wait_recv()

    def await_relay(e, side, pieces):
        for d in range(2):

            @when_side(side, x_there[d])
            def _(d=d):
                for j in pieces:
                    relay(e, side, j, 1 - d if side else d).wait_recv()

    def await_x(e, pairs):
        for d in range(2):

            @pl.when(x_there[d])
            def _(d=d):
                for pair in pairs:
                    x_copy(e, pair, 1 - d).wait_recv()
                    j = NY // 2 - pair
                    if j < reach(e):
                        relay(e, 0, j, d).start()

    def drain(e):
        for side in range(2):
            for j in pieces_of(e, side):
                if side == 0 or e != 2:
                    when_side(side)(lambda j=j, side=side: y_copy(e, side, j).wait_send())
                else:

                    @pl.when(far_there & (band == (j - 1) % 4))
                    def _(j=j):
                        y_copy(e, 1, j).wait_send()
                        for i in range(1, n_band):
                            spread(j, i).wait_send()

            for d in range(2):

                @when_side(side, x_there[d])
                def _(side=side, d=d):
                    for j in relays_of(e, side):
                        relay(e, side, j, d).wait_send()

        for d in range(2):

            @pl.when(x_there[d])
            def _(d=d):
                for pair in range(NY // 2):
                    x_copy(e, pair, d).wait_send()

    def band_rows(t, whose, pair):
        return D.at[t, whose, pl.ds(0, NX), pl.ds(row_of(pair) - HY, 2)]

    def band_copy(t, pair, i):
        part = band_rows(t, band, pair)
        return remote(part, part, bs.at[t, pair, i - 1], br.at[t, pair, i - 1], at(b=lax.rem(band + i, n_band)))

    def band_from(t, pair, i):
        other = lax.rem(band + n_band - i, n_band)
        part = band_rows(t, other, pair)
        return remote(part, part, bs.at[t, pair, i - 1], br.at[t, pair, i - 1], at(b=other))

    def send_band(t, pair):
        for i in range(1, n_band):
            band_copy(t, pair, i).start()

    def unit(t, k, pair, width):
        src, dst = (t if k == 1 else k), k + 1
        y0, x0 = row_of(pair), H + NX // 2 - width // 2
        u = {}
        for dx in range(-2, width + 2):
            for dy in range(-2, 4):
                if 0 <= dx < width or 0 <= dy < 2:
                    u[dx, dy] = S[src, x0 + dx, y0 + dy]
        stack = jnp.concatenate([u[dx, dy] for dx in range(width) for dy in range(2)], axis=0)
        high = stack.astype(jnp.bfloat16)
        low = (stack - high.astype(jnp.float32)).astype(jnp.bfloat16)
        along = jnp.dot(
            jnp.concatenate([high, low], axis=1), Z[...], preferred_element_type=jnp.float32
        )
        for dx in range(width):
            for dy in range(2):
                one = (u[dx - 1, dy] + u[dx + 1, dy]) + (u[dx, dy - 1] + u[dx, dy + 1])
                two = (u[dx - 2, dy] + u[dx + 2, dy]) + (u[dx, dy - 2] + u[dx, dy + 2])
                at_cell = F * (2 * dx + dy)
                around = (two + along[at_cell : at_cell + F]) - 16.0 * one
                S[dst, x0 + dx, y0 + dy] = V[t, x0 + dx, y0 + dy] * u[dx, dy] + far_w * around
        if width > NX:
            for d, edge in ((0, H - 2), (1, H + NX)):

                @pl.when(jnp.logical_not(x_there[d]))
                def _(edge=edge):
                    for dx in range(2):
                        for dy in range(2):
                            S[dst, edge + dx, y0 + dy] = zero

    def stage(t, j, after=False):
        if after:
            for k in range(1, 5):
                unit(t, k, k, NX + 4 * (4 - k))
            return
        if j < 1:
            for k in range(1, 5):

                def one_pair(pair, carry, k=k):
                    unit(t, k, pair, NX + 4 * (4 - k))
                    return carry

                lax.fori_loop(k - j, 10 - k, one_pair, 0)
            return

        def some(ks, j=j):
            for k in ks:
                unit(t, k, k - j, NX + 4 * (4 - k - max(j - k - (0 if t else M), 0)))

        if j > 1:
            pl.when(far_there)(lambda: some(range(1, min(j, 5))))
        some(range(j, 5))

    sub = lax.broadcasted_iota(jnp.int32, (F, NZ), 0)
    sign = jnp.where(sub < F // 2, 1.0, -1.0)

    def combine(s, w):
        even = w[0] + ((s**4 / 24.0) * w[4] - (s**2 / 2.0) * w[2])
        odd_part = s * w[1] - (s**3 / 6.0) * w[3]
        return even + sign * pltpu.roll(odd_part, F // 2, 0)

    def each_of(pair, body):
        y0 = row_of(pair)

        def step(i, carry):
            for dx in range(4):
                for dy in range(2):
                    body(4 * i + dx, y0 - HY + dy)
            return carry

        lax.fori_loop(0, NX // 4, step, 0)

    def terms(t, x, y):
        return [S[t, H + x, HY + y]] + [S[k, H + x, HY + y] for k in range(2, 6)]

    def half_way(x, y):
        w = terms(0, x, y)
        D[1, band, x, y] = density_of(combine(step_length, w))
        S[1, H + x, HY + y] = combine(step_length / 2, w)

    def half_way_only(x, y):
        S[1, H + x, HY + y] = combine(step_length / 2, terms(0, x, y))

    def half_halo_row(pair):
        @pl.when(far_there)
        def _():
            each_of(pair, half_way_only)
            for d in range(2):
                pl.when(x_there[d])(lambda d=d: relay(1, 1, -pair, d).start())

    def half_row(pair):
        each_of(pair, half_way)
        send_band(1, pair)
        if M <= pair < 4:
            send_y(1, 1, [pair + 1])
        if pair > 1:
            send_y(1, 0, [6 - pair])
        send_x(1, [pair])

    def take_out(x, y):
        out[pl.ds(y * NX + x, F, stride=NX * NY), :] = combine(step_length / 2, terms(1, x, y))

    def out_row(pair):
        each_of(pair, take_out)

    def potential_row(t, pair):
        for i in range(1, n_band):
            band_from(t, pair, i).wait_recv()

        def cell(x, y):
            total = (D[t, 0, x, y] + D[t, 1, x, y]) + (D[t, 2, x, y] + D[t, 3, x, y])
            v = ext[pl.ds(y * NX + x, 1), :] - exchange_coef * cube_root(total)
            if t == 1:
                pot[pl.ds(y * NX + x, 1), :] = v
            V[t, H + x, HY + y] = v + centre

        each_of(pair, cell)
        if pair + 1 in pieces_of(t + 2, 1):
            mine = far_there & (band == pair % 4) if t == 0 else far_there
            pl.when(mine)(lambda: y_copy(t + 2, 1, pair + 1).start())
        if pair > 2:
            send_y(t + 2, 0, [6 - pair])
        send_x(t + 2, [pair])

    scope = jax.named_scope
    rows = range(NY // 2)

    send_y(0, 1, [1, 2])
    for pair in rows:
        send_band(0, pair)
    send_y(0, 0, range(1, 5))
    send_x(0, rows)
    with scope('pot0'):
        for pair in rows:
            potential_row(0, pair)
    send_y(0, 1, range(3, 5 + M))
    with scope('far01'):
        take_far(0, [1])
    with scope('x0'):
        await_x(0, rows)
        await_x(2, rows)
    with scope('near0'):
        await_near(0)
        await_near(2)
        await_relay(0, 0, relays_of(0, 0))
        await_relay(2, 0, relays_of(2, 0))
    with scope('far02'):
        take_far(0, [2])
    with scope('stage00'):
        stage(0, 0)
    with scope('half00'):
        half_row(5)
        half_row(4)
    for j in range(1, 5 + M):
        with scope(f'far0{j}'):
            if j in relays_of(0, 1):
                if j > 1 and j + 1 in relays_of(0, 1):
                    take_far(0, [j + 1])
            else:
                take_far(0, [j])
            if j in pieces_of(2, 1):
                take_far_potential([j])
        with scope(f'farrelay0{j}'):
            if j in relays_of(0, 1):
                await_relay(0, 1, [j])
            if j - 1 in relays_of(2, 1):
                await_relay(2, 1, [j - 1])
        with scope(f'stage0{j}'):
            stage(0, j)
            if j < 5:
                half_row(4 - j)
            else:
                half_halo_row(4 - j)
        with scope(f'pot1{j}'):
            if j == 1:
                potential_row(1, 5)
                potential_row(1, 4)
            elif j < 5:
                potential_row(1, 5 - j)
            if j == 4:
                potential_row(1, 0)

    with scope('far1a'):
        take_far(1, range(4, max(M, 1), -1))
    with scope('near1'):
        await_x(1, [5, 4, 3, 2])
        await_x(3, [5, 4, 3, 2])
        await_near(1)
        await_near(3)
        await_x(1, [1])
        await_x(3, [1])
        await_relay(1, 0, relays_of(1, 0))
        await_relay(3, 0, relays_of(3, 0))
    with scope('stage1m'):
        stage(1, -1)
        out_row(5)
    with scope('x1'):
        await_x(1, [0])
    with scope('farV1'):
        take_far(1, [1])
        take_far(3, [2, 1, 3])
    with scope('stage10'):
        stage(1, 0, after=True)
        out_row(4)
    with scope('farrelay1'):
        await_x(3, [0])
        await_relay(1, 1, relays_of(1, 1))
    with scope('stage11'):
        stage(1, 1)
        out_row(3)
    with scope('farrelayV1'):
        await_relay(3, 1, relays_of(3, 1))
    with scope('stages1'):
        for j in range(2, 5):
            stage(1, j)
            out_row(4 - j)
    with scope('drain'):
        for t in range(2):
            for pair in rows:
                for i in range(1, n_band):
                    band_copy(t, pair, i).wait_send()
            drain(t)
            drain(t + 2)


def body(orbitals, external):
    rows = NX * NY
    vmem = pl.BlockSpec(memory_space=pltpu.VMEM)
    dma = pltpu.SemaphoreType.DMA
    out, pot = pl.pallas_call(
        kernel,
        out_shape=(
            jax.ShapeDtypeStruct((F * rows, NZ), jnp.float32),
            jax.ShapeDtypeStruct((rows, NZ), jnp.float32),
        ),
        in_specs=[pl.BlockSpec(memory_space=pltpu.HBM)] * 2,
        out_specs=(vmem, vmem),
        scratch_shapes=[
            pltpu.VMEM((6, EX, EY, F, NZ), jnp.float32),
            pltpu.VMEM((2, EX, EY, 1, NZ), jnp.float32),
            pltpu.VMEM((2, 4, NX, NY, 1, NZ), jnp.float32),
            pltpu.VMEM((2 * NZ, NZ), jnp.bfloat16),
            pltpu.VMEM((F * rows, NZ), jnp.float32),
            pltpu.VMEM((rows, NZ), jnp.float32),
            dma((4, 2, 4 + M)),
            dma((4, 2, 4 + M)),
            dma((4, 6, 2)),
            dma((4, 6, 2)),
            dma((4, 2, 3 + M, 2)),
            dma((4, 2, 3 + M, 2)),
            dma((2, 6, 3)),
            dma((2, 6, 3)),
            dma((3 + M, 3)),
            dma((3 + M,)),
            dma((2,)),
        ],
        compiler_params=pltpu.CompilerParams(
            collective_id=0, has_side_effects=True, vmem_limit_bytes=40 * 1024 * 1024
        ),
        name="etrs",
    )(
        pltpu.with_memory_space_constraint(orbitals.transpose(0, 1, 3, 2, 4).reshape(F * rows, NZ), pltpu.HBM),
        pltpu.with_memory_space_constraint(external.transpose(1, 0, 2).reshape(rows, NZ), pltpu.HBM),
    )
    out = out.reshape(2, F // 2, NY, NX, NZ).transpose(0, 1, 3, 2, 4)
    return out, pot.reshape(NY, NX, NZ).transpose(1, 0, 2)


def solution(mesh):
    in_specs = (P(None, "band", "gx", "gy", None), P("gx", "gy", None))
    out_specs = (P(None, "band", "gx", "gy", None), P("gx", "gy", None))
    return jax.shard_map(body, mesh=mesh, in_specs=in_specs, out_specs=out_specs, check_vma=False)
```
